32 devices in a mesh: dp: 16 (over z, x, core), tensor: 2 (over y).
Axes of the slice: x: 2, y: 2, z: 4, core: 2. Of those that a mesh axis runs over, the one named last changes fastest.
Arguments:
- hidden: bfloat16 [5120, 18432], P('dp', 'tensor'), may hold values from -6 to 6
- fixed_down_weight: bfloat16 [18432, 4608], P('tensor', 'dp'), may hold values from -4 to 4
- lowrank_factor_b: bfloat16 [18432, 16], P('tensor'), may hold values from -0.046875 to 0.046875
- lowrank_factor_a: bfloat16 [16, 4608], P(None, 'dp'), may hold values from -1.5 to 1.5
- magnitude: float32 [4608], P('tensor'), may hold values from 0.5 to 2
- cotangent: bfloat16 [5120, 4608], P('dp', 'tensor'), may hold values from -0.083496094 to 0.083496094
Outputs:
- mixed: bfloat16 [5120, 4608], P('dp', 'tensor')
- gradient_column_scale: float32 [4608], P(('tensor', 'dp'))
- gradient_factor_a: float32 [16, 4608], P(None, ('tensor', 'dp'))
- gradient_factor_b: float32 [18432, 16], P(('tensor', 'dp'))
The draws below stay inside these ranges and needn't reach their ends.
All inputs are finite; a program needn't handle non-finite values.
Results may differ from the reference program's by a relative error of at most 0.0054.
Values may be sent and summed in bfloat16 or wider, within the bound.
No kernel may reach another device: no remote copies, remote signals or barrier semaphores. Data moves between devices by JAX's collectives and lax.ppermute only.
A program may use at most 192 MiB of HBM per device.

```python
import math
import jax
import jax.numpy as jnp
from jax import lax

MODEL_WIDTH = 4608
HALF_FEEDFORWARD = 18432
ADAPTER_RANK = 16
TOK_DEV = 320
TOKENS = 5120
N_DP = 16


def draw_fixed_down_weight(key, part):
    base = jax.random.truncated_normal(key, -4.0, 4.0, (HALF_FEEDFORWARD, MODEL_WIDTH), jnp.float32) * HALF_FEEDFORWARD ** (-0.5)
    ramp = 0.5 + jnp.arange(HALF_FEEDFORWARD, dtype=jnp.float32) / (HALF_FEEDFORWARD - 1)
    return (base * ramp[:, None]).astype(jnp.bfloat16)


def raised(array, rng, source, target, shards_of, factor):
    owner, partner = [(jnp.arange(array.shape[dim]) // (array.shape[dim] // shards_of)).reshape([-1 if axis == dim else 1 for axis in range(array.ndim)]) for dim in (source, target)]
    chosen = jax.random.permutation(rng, shards_of)[partner]
    strong = (owner == chosen) | (owner == (partner + shards_of // 2) % shards_of)
    return jnp.where(strong, factor * array, array)


def levels(key, extent, shards, low, largest):
    factor_of = 1.0
    for axis_at, shards_of in shards:
        steps = jax.random.uniform(jax.random.fold_in(jax.random.fold_in(key, 6), axis_at), (shards_of,), jnp.float32, low / len(shards), largest / len(shards))
        factor_of = factor_of * jnp.repeat(jnp.exp(steps), extent[axis_at] // shards_of).reshape((-1,) + (1,) * (len(extent) - 1 - axis_at))
    return factor_of


def normal_values(rng, extent, deviation, limit, pieces=(), held_as=jnp.bfloat16):
    gain = levels(rng, extent, pieces, -0.22, 0.18) if pieces else 1.0
    values = jax.random.normal(rng, extent, jnp.float32) * deviation * gain
    return jnp.minimum(jnp.maximum(values, -limit), limit).astype(held_as)


def bell_draw_with(own_key, extent, spread, bound, cuts, heavy, held_as=jnp.bfloat16):
    array = spread * jax.random.normal(own_key, extent, jnp.float32)
    if cuts:
        array = array * levels(own_key, extent, cuts, -0.22, 0.18)
    return jnp.clip(raised(array, jax.random.fold_in(own_key, 3), *heavy), -bound, bound).astype(held_as)


def setup_inputs(seed: int = 0) -> dict:
    arg_keys = jax.random.split(jax.random.key(seed), 7)
    return {
        "hidden": bell_draw_with(arg_keys[0], (TOKENS, HALF_FEEDFORWARD), 1.0, 6.0, ((0, 16), (1, 2)), (0, 1, 16, 2.0)),
        "fixed_down_weight": draw_fixed_down_weight(jax.random.fold_in(arg_keys[6], 71), 0),
        "lowrank_factor_b": normal_values(arg_keys[2], (HALF_FEEDFORWARD, ADAPTER_RANK), HALF_FEEDFORWARD ** -0.5, 0.046875, ((0, 2),)),
        "lowrank_factor_a": normal_values(arg_keys[3], (ADAPTER_RANK, MODEL_WIDTH), ADAPTER_RANK ** -0.5, 1.5, ((1, 16),)),
        "magnitude": jnp.clip(jnp.exp(math.log(2.0) - 1.3862944 * jax.random.uniform(arg_keys[4], (MODEL_WIDTH,), jnp.float32) ** levels(arg_keys[4], (MODEL_WIDTH,), ((0, 2),), -0.2, 0.2)), 0.5, 2.0),
        "cotangent": bell_draw_with(arg_keys[5], (TOKENS, MODEL_WIDTH), ((TOK_DEV * N_DP) ** -0.5), 0.083496094, ((0, 16), (1, 2)), (0, 1, 16, 2.0)),
    }


def squared_column_entries(fixed_down_weight, lowrank_factor_b, lowrank_factor_a):
    w_blocks = fixed_down_weight.reshape(8, HALF_FEEDFORWARD // 8, MODEL_WIDTH)
    factor_b_blocks = lowrank_factor_b.reshape(8, HALF_FEEDFORWARD // 8, ADAPTER_RANK)

    def one_block(pair):
        weight_tile_block, factor_b_block = pair
        combined_weight = weight_tile_block.astype(jnp.float32) + jnp.dot(factor_b_block, lowrank_factor_a, preferred_element_type=jnp.float32)
        return lax.optimization_barrier(jnp.sum(combined_weight * combined_weight, axis=0))
    return lax.optimization_barrier(jnp.sum(lax.map(one_block, (w_blocks, factor_b_blocks)), axis=0))

def reference(hidden, fixed_down_weight, lowrank_factor_b, lowrank_factor_a, magnitude, cotangent):
    column_norm_values = jnp.sqrt(squared_column_entries(fixed_down_weight, lowrank_factor_b, lowrank_factor_a) + 1e-06)
    scale = magnitude / column_norm_values
    lowrank_update = jnp.dot(hidden, lowrank_factor_b, preferred_element_type=jnp.float32)
    lowrank_block_update = lowrank_update.astype(jnp.bfloat16)
    prenorm_output = jnp.dot(hidden, fixed_down_weight, preferred_element_type=jnp.float32) + jnp.dot(lowrank_block_update, lowrank_factor_a, preferred_element_type=jnp.float32)
    mixed = (prenorm_output * scale).astype(jnp.bfloat16)
    cot = cotangent.astype(jnp.float32)
    gradient_column_scale = lax.optimization_barrier(jnp.sum(cot * prenorm_output, axis=0)) / column_norm_values
    prenorm_gradient_b = (cot * scale).astype(jnp.bfloat16)
    gradient_factor_a = jnp.dot(lowrank_block_update.T, prenorm_gradient_b, preferred_element_type=jnp.float32)
    backward_factor_b = jnp.dot(prenorm_gradient_b, lowrank_factor_a.T, preferred_element_type=jnp.float32).astype(jnp.bfloat16)
    gradient_factor_b = jnp.dot(hidden.T, backward_factor_b, preferred_element_type=jnp.float32)
    return (mixed, gradient_column_scale, gradient_factor_a, gradient_factor_b)
```

```python
import jax
import jax.numpy as jnp
from jax import lax
from jax.sharding import PartitionSpec as P

def routed_products(hidden, weight, n_dp, n_tensor):
    far, near, side, core = n_dp // 2, n_dp // 4, n_dp // 8, n_dp // 16

    def swap(v, mask):
        return lax.ppermute(v, "dp", [(s, s ^ mask) for s in range(n_dp)])

    def flat(i, t):
        return i * n_tensor + t

    def half_of(i):
        return i // far

    def over_tensor(v, to_own):
        pairs = []
        for i in range(n_dp):
            dst = half_of(i) if to_own else 1 - half_of(i)
            pairs.append((flat(i, 1 - dst), flat(i, dst)))
        return lax.ppermute(v, ("dp", "tensor"), pairs)

    def home(v, mask, own):
        pairs = []
        for i in range(n_dp):
            t = half_of(i) if own else 1 - half_of(i)
            pairs.append((flat(i, t), flat(i ^ mask, t)))
        return lax.ppermute(v, ("dp", "tensor"), pairs)

    index = lax.axis_index("dp")
    owns_near = lax.axis_index("tensor") == index // far
    tokens, units = hidden.shape
    cols = weight.shape[1]
    wt = weight.T
    COL_CUTS, UNIT_CUTS = 2, 2
    cc, uc = cols // COL_CUTS, units // UNIT_CUTS

    h_near = swap(hidden, near)
    w_side = swap(wt, side)
    far_pieces = [
        [swap(wt[j * cc:(j + 1) * cc, k * uc:(k + 1) * uc], far) for k in range(UNIT_CUTS)]
        for j in range(COL_CUTS)
    ]
    h_core = swap(hidden, core)
    h_both = swap(h_near, core)
    rows = jnp.concatenate([hidden, h_core, h_near, h_both], axis=0)
    masks = [0, core, near, near + core]

    def by_block(v):
        return [v[r * tokens:(r + 1) * tokens] for r in range(len(masks))]

    def mul(x, w):
        return lax.dot_general(x, w, (((1,), (1,)), ((), ())), preferred_element_type=jnp.float32)

    w_own = jnp.concatenate([wt, w_side], axis=0)
    p_own = mul(rows, w_own)
    got = over_tensor(p_own.astype(jnp.bfloat16), True)
    own_sum = by_block((p_own + got.astype(jnp.float32)).astype(jnp.bfloat16))
    own_home = [own_sum[0]] + [home(own_sum[r], masks[r], True) for r in (1, 2, 3)]

    far_home = []
    for j in range(COL_CUTS):
        crossed = [swap(piece, side) for piece in far_pieces[j]]
        w_far = [jnp.concatenate(pair, axis=0) for pair in zip(far_pieces[j], crossed)]
        p_far = sum(mul(rows[:, k * uc:(k + 1) * uc], w_far[k]) for k in range(UNIT_CUTS))
        got = over_tensor(p_far.astype(jnp.bfloat16), False)
        far_sum = by_block((p_far + got.astype(jnp.float32)).astype(jnp.bfloat16))
        far_home.append([far_sum[0]] + [home(far_sum[r], masks[r], False) for r in (1, 2, 3)])

    blocks = [None] * (2 * len(masks))
    for r, mask in enumerate(masks):
        for q in range(2):
            from_far = jnp.concatenate([far_home[j][r][:, q * cc:(q + 1) * cc] for j in range(COL_CUTS)], axis=1)
            from_own = own_home[r][:, q * cols:(q + 1) * cols]
            blocks[mask + q * side] = jnp.where(owns_near, from_own, from_far)
    stacked = jnp.stack(blocks)
    me = index % far
    return jnp.concatenate(
        [lax.dynamic_index_in_dim(stacked, p ^ me, 0, False) for p in range(far)], axis=1
    ).astype(jnp.float32), far_pieces[-1][-1]


def gathered_body(hidden, fixed_down_weight, lowrank_factor_b, lowrank_factor_a, magnitude, cotangent):
    out_cols = magnitude.shape[0]
    own = lax.axis_index("tensor")
    lowrank_portion = jnp.dot(hidden, lowrank_factor_b, preferred_element_type=jnp.float32)
    combined_weight = fixed_down_weight.astype(jnp.float32) + jnp.dot(
        lowrank_factor_b, lowrank_factor_a, preferred_element_type=jnp.float32
    )
    local_sq = jnp.sum(combined_weight * combined_weight, axis=0)
    low_full, block_sq = lax.psum((lowrank_portion, local_sq), "tensor")
    col_sq = lax.all_gather(block_sq, "dp", axis=0, tiled=True)
    sq_len = 1
    weight_shape = (1, 1)
    squares = jnp.zeros((sq_len,), jnp.float32)
    full_w = jnp.zeros(weight_shape, jnp.bfloat16)
    w_piece = lax.all_gather(fixed_down_weight, "dp", axis=1, tiled=True)
    factor_a_slice = lax.all_gather(lowrank_factor_a, "dp", axis=1, tiled=True)
    products = jnp.dot(hidden, w_piece, preferred_element_type=jnp.float32)
    full_a = factor_a_slice
    products, squares, full_a, full_w = (products, squares, full_a, full_w)
    column_norm_values = jnp.sqrt(col_sq + 1e-06)
    own_norms = lax.dynamic_slice_in_dim(column_norm_values, own * out_cols, out_cols, 0)
    scale = magnitude / own_norms
    lowrank_block_update = low_full.astype(jnp.bfloat16)
    summed = lax.psum_scatter(products, "tensor", scatter_dimension=1, tiled=True)
    own_a = lax.dynamic_slice_in_dim(full_a, own * out_cols, out_cols, 1)
    prenorm_output = summed + jnp.dot(
        lowrank_block_update, own_a, preferred_element_type=jnp.float32
    )
    mixed = (prenorm_output * scale).astype(jnp.bfloat16)
    cot = cotangent.astype(jnp.float32)
    mag_part = jnp.sum(cot * prenorm_output, axis=0) / own_norms
    prenorm_gradient_b = (cot * scale).astype(jnp.bfloat16)
    factor_a_portion = jnp.dot(
        lowrank_block_update.T, prenorm_gradient_b, preferred_element_type=jnp.float32
    )
    back_part = jnp.dot(prenorm_gradient_b, own_a.T, preferred_element_type=jnp.float32)
    backward_factor_b = lax.psum(back_part, "tensor").astype(jnp.bfloat16)
    b_part = jnp.dot(hidden.T, backward_factor_b, preferred_element_type=jnp.float32)
    gradient_column_scale, gradient_factor_b = (
        lax.psum_scatter(mag_part, "dp", scatter_dimension=0, tiled=True),
        lax.psum_scatter(b_part, "dp", scatter_dimension=0, tiled=True),
    )
    gradient_factor_a = lax.psum_scatter(factor_a_portion, "dp", scatter_dimension=1, tiled=True)
    return (mixed, gradient_column_scale, gradient_factor_a, gradient_factor_b)


def exchanges(n_dp, n_tensor):
    index = lax.axis_index("dp")

    def swap(v, mask):
        return lax.ppermute(v, "dp", [(s, s ^ mask) for s in range(n_dp)])

    def add_halves(v):
        return v + lax.ppermute(v, "tensor", [(s, s ^ 1) for s in range(n_tensor)])

    def gather_low(v, limit):
        mask = 1
        while mask < limit:
            other = swap(v, mask)
            upper = (index // mask) % 2 == 1
            v = jnp.where(upper, jnp.concatenate([other, v], 0), jnp.concatenate([v, other], 0))
            mask *= 2
        return v

    def scatter_sum(v):
        mask = n_dp // 2
        while mask:
            half = v.shape[1] // 2
            upper = (index // mask) % 2 == 1
            low, high = v[:, :half], v[:, half:]
            v = jnp.where(upper, high, low) + swap(jnp.where(upper, low, high), mask)
            mask //= 2
        return v

    return swap, add_halves, gather_low, scatter_sum


def make_routed_body(n_dp, n_tensor):
    def body(hidden, fixed_down_weight, lowrank_factor_b, lowrank_factor_a, magnitude, cotangent):
        swap, add_halves, gather_low, scatter_sum = exchanges(n_dp, n_tensor)
        far = n_dp // 2
        rank = lowrank_factor_a.shape[0]
        own = lax.axis_index("tensor")
        owns_near = own == lax.axis_index("dp") // far
        combined_weight = fixed_down_weight.astype(jnp.float32) + jnp.dot(
            lowrank_factor_b, lowrank_factor_a, preferred_element_type=jnp.float32
        )
        block_sq = add_halves(jnp.sum(combined_weight * combined_weight, axis=0)[None, :])
        block = jnp.concatenate([lowrank_factor_a.astype(jnp.float32), block_sq], axis=0)
        block = jnp.where(owns_near, block, swap(block, far))
        columns = gather_low(block[None], far)
        columns = jnp.concatenate([columns[p] for p in range(far)], axis=1)
        low_full = add_halves(jnp.dot(hidden, lowrank_factor_b, preferred_element_type=jnp.float32))
        hidden_bulk, weight_bulk, columns, low_full = lax.optimization_barrier(
            (hidden, fixed_down_weight, columns, low_full)
        )
        summed, last = routed_products(hidden_bulk, weight_bulk, n_dp, n_tensor)
        own_a = columns[:rank].astype(jnp.bfloat16)
        own_norms = jnp.sqrt(columns[rank] + 1e-06)
        scale = magnitude / own_norms
        lowrank_block_update = low_full.astype(jnp.bfloat16)
        cot = cotangent.astype(jnp.float32)

        late_scale, late_low, last = lax.optimization_barrier((scale, lowrank_block_update, last))
        prenorm_gradient_b = (cot * late_scale).astype(jnp.bfloat16)
        factor_a_portion = jnp.dot(late_low.T, prenorm_gradient_b, preferred_element_type=jnp.float32)
        back = add_halves(jnp.dot(prenorm_gradient_b, own_a.T, preferred_element_type=jnp.float32))
        b_part = jnp.dot(back.astype(jnp.bfloat16).T, hidden, preferred_element_type=jnp.float32)
        gradient_factor_b = scatter_sum(b_part).T
        gradient_factor_a = scatter_sum(factor_a_portion)

        prenorm_output = summed + jnp.dot(
            lowrank_block_update, own_a, preferred_element_type=jnp.float32
        )
        mixed = (prenorm_output * scale).astype(jnp.bfloat16)
        mag_part = jnp.sum(cot * prenorm_output, axis=0) / own_norms
        gradient_column_scale = scatter_sum(mag_part[None, :])[0]
        return (mixed, gradient_column_scale, gradient_factor_a, gradient_factor_b)

    return body


def make_body(n_dp, n_tensor):
    if n_tensor == 2 and n_dp == n_tensor ** 4:
        return make_routed_body(n_dp, n_tensor)
    return gathered_body


def solution(mesh):
    return jax.shard_map(
        make_body(mesh.shape["dp"], mesh.shape["tensor"]),
        mesh=mesh,
        in_specs=(
            P("dp", "tensor"),
            P("tensor", "dp"),
            P("tensor", None),
            P(None, "dp"),
            P("tensor"),
            P("dp", "tensor"),
        ),
        out_specs=(
            P("dp", "tensor"),
            P(("tensor", "dp")),
            P(None, ("tensor", "dp")),
            P(("tensor", "dp"), None),
        ),
        check_vma=False,
    )
```
